256 devices in a mesh: trial: 4 (over z_lo), south: 4 (over y_lo, core), east: 4 (over x), down: 4 (over z_hi, y_hi).
Axes of the slice: x: 4, y: 4 (y_hi: 2, y_lo: 2; y = y_hi * 2 + y_lo), z: 8 (z_hi: 2, z_lo: 4; z = z_hi * 4 + z_lo), core: 2. Of those that a mesh axis runs over, the one named last changes fastest.
Arguments:
- tracer: float32 [64, 64, 512, 128], P(('trial', 'south'), 'east', 'down'), parts along dimension 0, may hold values from 0.5 to 2
- mobility: float32 [64, 64, 512, 128], P(('trial', 'south'), 'east', 'down'), parts along dimension 0, may hold values from 0.03 to 0.15
- source: float32 [64, 64, 512, 128], P(('trial', 'south'), 'east', 'down'), parts along dimension 0, may hold values from -0.2 to 0.2
Outputs:
- standardized: float32 [64, 64, 512, 128], P(('trial', 'south'), 'east', 'down'), parts along dimension 0
- tracer_end: float32 [64, 64, 512, 128], P(('trial', 'south'), 'east', 'down'), parts along dimension 0
The draws below stay inside these ranges and needn't reach their ends.
There are 4 independent parts, one for each index of `trial`. The reference program is written for one: setup_inputs(seed, part) draws one part's arguments, and reference() takes and returns one part's arrays. A program takes and returns all parts, laid end to end along the dimension named above; each array names one. Nothing has to cross between parts.
All inputs are finite; a program needn't handle non-finite values.
Results may differ from the reference program's by a relative error of at most 0.00002.
Values sent between devices are 32-bit elements; how exact they have to be, the bound alone decides.
A program may use at most 128 MiB of HBM per device.

```python
import jax
import jax.numpy as jnp
from jax import lax

GRID_Y = 16
GRID_X = 64
GRID_Z = 512
LEVELS = 128
STEPS = 3


def level_of(stream_key, shape, split, least, top_value):
    level = 1.0
    for axis_at, shards_of in split:
        heights = jax.random.uniform(jax.random.fold_in(jax.random.fold_in(stream_key, 6), axis_at), (shards_of,), jnp.float32, least / len(split), top_value / len(split))
        level = level * jnp.repeat(jnp.exp(heights), shape[axis_at] // shards_of).reshape((-1,) + (1,) * (len(shape) - 1 - axis_at))
    return level


def setup_inputs(seed: int = 0, part: int = 0) -> dict:
    arg_keys = jax.random.split(jax.random.key(seed), 4)
    part_keys = jax.random.split(jax.random.fold_in(arg_keys[3], part), 4)
    tracer = jnp.clip(0.5 + 1.5 * jax.random.uniform(part_keys[0], (GRID_Y, GRID_X, GRID_Z, LEVELS), jnp.float32) ** level_of(part_keys[0], (GRID_Y, GRID_X, GRID_Z, LEVELS), ((0, 4), (1, 4), (2, 4)), -0.2, 0.2), 0.5, 2.0)
    mobility = jnp.clip(0.03 + 0.120000007 * jax.random.uniform(part_keys[1], (GRID_Y, GRID_X, GRID_Z, LEVELS), jnp.float32) ** level_of(part_keys[1], (GRID_Y, GRID_X, GRID_Z, LEVELS), ((0, 4), (1, 4), (2, 4)), -0.2, 0.2), 0.03, 0.15)
    source = jnp.clip(jax.random.uniform(part_keys[2], (GRID_Y, GRID_X, GRID_Z, LEVELS), jnp.float32, -0.2, 0.2) * level_of(part_keys[2], (GRID_Y, GRID_X, GRID_Z, LEVELS), ((0, 4), (1, 4), (2, 4)), -0.4, 0.0), -0.2, 0.2)
    return dict(tracer=tracer, mobility=mobility, source=source)


def strip_edges(values, dims):
    for dim in dims:
        values = lax.slice_in_dim(values, 1, values.shape[dim] - 1, axis=dim)
    return values

def neighbour(values, dim, start, dims):
    others = [other for other in dims if other != dim]
    values = strip_edges(values, others)
    return lax.slice_in_dim(values, start, start + values.shape[dim] - 2, axis=dim)

def one_step(padded, mobility, source):
    middle = strip_edges(padded, (0, 1, 2))
    lower = [neighbour(padded, dim, 0, (0, 1, 2)) for dim in (0, 1, 2)]
    upper = [neighbour(padded, dim, 2, (0, 1, 2)) for dim in (0, 1, 2)]
    spread = lower[0] + upper[0] + lower[1] + upper[1] + lower[2] + upper[2] - 6.0 * middle
    return middle + mobility * spread + source

def reference(tracer, mobility, source):
    for step in range(STEPS):
        tracer = one_step(jnp.pad(tracer, ((1, 1), (1, 1), (1, 1), (0, 0)), mode='wrap'), mobility, source)
    line_mean = lax.optimization_barrier(jnp.mean(tracer, axis=2, keepdims=True))
    centred = tracer - line_mean
    line_variance = lax.optimization_barrier(jnp.mean(centred * centred, axis=2, keepdims=True))
    standardized = centred * lax.rsqrt(line_variance + 0.0001)
    return (standardized, tracer)
```

```python
import functools

import jax
import jax.numpy as jnp
from jax import lax
from jax.experimental import pallas as pl
from jax.experimental.pallas import tpu as pltpu
from jax.sharding import PartitionSpec as P

STEPS = 3
AHEAD = 4
LAG = 3
MESH = pl.DeviceIdType.MESH


def kernel(
    sizes,
    tr, mo, so,
    std_o, tr_o,
    u, m, s, st, zs, zr, ms, mr,
    in_sem, out_sem,
    s_send, s_recv, e_send, e_recv, z_send, z_recv, m_send, m_recv,
):
    souths, easts, downs = sizes
    Y, X, Z, L = tr.shape
    pairs = X // 2
    rows = 2 * Y
    at = {name: lax.axis_index(name) for name in ("south", "east", "down")}

    def peer(name, count, shift):
        return {name: lax.rem(at[name] + shift + count, count)}

    def south(side, t, x):
        return pltpu.make_async_remote_copy(
            src_ref=u.at[t, Y if side else 1, x + 1],
            dst_ref=u.at[t, 0 if side else Y + 1, x + 1],
            send_sem=s_send.at[side, t, x],
            recv_sem=s_recv.at[side, t, x],
            device_id=peer("south", souths, 1 if side else -1),
            device_id_type=MESH,
        )

    def east(side, t):
        return pltpu.make_async_remote_copy(
            src_ref=u.at[t, pl.ds(1, Y), X if side else 1],
            dst_ref=u.at[t, pl.ds(1, Y), 0 if side else X + 1],
            send_sem=e_send.at[side, t],
            recv_sem=e_recv.at[side, t],
            device_id=peer("east", easts, 1 if side else -1),
            device_id_type=MESH,
        )

    def down(side, t, j):
        return pltpu.make_async_remote_copy(
            src_ref=zs.at[t, side, j],
            dst_ref=zr.at[t, side, j],
            send_sem=z_send.at[side, t, j],
            recv_sem=z_recv.at[side, t, j],
            device_id=peer("down", downs, 1 if side else -1),
            device_id_type=MESH,
        )

    def moments(d, j):
        return pltpu.make_async_remote_copy(
            src_ref=ms.at[j],
            dst_ref=mr.at[d - 1, j],
            send_sem=m_send.at[d - 1, j],
            recv_sem=m_recv.at[d - 1, j],
            device_id=peer("down", downs, d),
            device_id_type=MESH,
        )

    def south_pair(t, j):
        for side in (0, 1):
            for x in (j, X - 1 - j):
                south(side, t, x).start()

    def save_line(t, y, x):
        return pltpu.make_async_copy(u.at[t, pl.ds(1, Y), x + 1], tr_o.at[:, x], out_sem.at[0, x])

    def save_std(x):
        return pltpu.make_async_copy(st.at[:, x], std_o.at[:, x], out_sem.at[1, x])

    loads = [
        pltpu.make_async_copy(tr.at[y], u.at[0, y + 1, pl.ds(1, X)], in_sem.at[y])
        for y in range(Y)
    ]
    for y in [0, Y - 1] + list(range(1, Y - 1)):
        loads[y].start()
    others = [
        pltpu.make_async_copy(mo, m, in_sem.at[Y]),
        pltpu.make_async_copy(so, s, in_sem.at[Y + 1]),
    ]
    for copy in others:
        copy.start()

    barrier = pltpu.get_barrier_semaphore()
    greet = [peer("south", souths, d) for d in (-1, 1)]
    greet += [peer("east", easts, d) for d in (-1, 1)]
    greet += [peer("down", downs, d) for d in range(1, downs)]
    for who in greet:
        pl.semaphore_signal(barrier, inc=1, device_id=who, device_id_type=MESH)
    pl.semaphore_wait(barrier, len(greet))

    for copy in loads:
        copy.wait()

    def first_faces(j, carry):
        for r, x in enumerate((j, X - 1 - j)):
            for y in range(Y):
                zs[0, 0, j, pl.ds(r * Y + y, 1), :] = u[0, y + 1, x + 1, pl.ds(0, 1), :]
                zs[0, 1, j, pl.ds(r * Y + y, 1), :] = u[0, y + 1, x + 1, pl.ds(Z - 1, 1), :]
        return carry

    lax.fori_loop(0, pairs, first_faces, 0)
    south_pair(0, 0)
    for side in (0, 1):
        east(side, 0).start()

    def first_down(j, carry):
        for side in (0, 1):
            down(side, 0, j).start()
        return carry

    lax.fori_loop(0, pairs, first_down, 0)
    for j in range(1, AHEAD):
        south_pair(0, j)
    for copy in others:
        copy.wait()

    level = lax.broadcasted_iota(jnp.int32, (Z, L), 0)
    top, bottom = level == 0, level == Z - 1

    def advance(t, j):
        for side in (0, 1):
            down(side, t, j).wait_recv()
            for x in (j, X - 1 - j):
                south(side, t, x).wait_recv()

        @pl.when(j == 0)
        def _():
            for side in (0, 1):
                east(side, t).wait_recv()

        for r, x in enumerate((j, X - 1 - j)):
            for y in range(Y):
                at_row = pl.ds(r * Y + y, 1)
                middle = u[t, y + 1, x + 1]
                before = jnp.where(top, zr[t, 1, j, at_row, :], pltpu.roll(middle, 1, 0))
                after = jnp.where(bottom, zr[t, 0, j, at_row, :], pltpu.roll(middle, Z - 1, 0))
                spread = u[t, y, x + 1] + u[t, y + 2, x + 1] + u[t, y + 1, x] + u[t, y + 1, x + 2]
                spread = spread + before + after - 6.0 * middle
                value = middle + m[y, x] * spread + s[y, x]
                u[t + 1, y + 1, x + 1] = value
                if t + 1 < STEPS:
                    zs[t + 1, 0, j, at_row, :] = value[:1]
                    zs[t + 1, 1, j, at_row, :] = value[Z - 1 :]
                else:
                    mean = jnp.sum(value, axis=0, keepdims=True) * (1.0 / Z)
                    off = value - mean
                    ms[j, 0, at_row, :] = mean
                    ms[j, 1, at_row, :] = jnp.sum(off * off, axis=0, keepdims=True)

    def finish(j):
        for d in range(1, downs):
            moments(d, j).wait_recv()
        means = [ms[j, 0]] + [mr[d, j, 0] for d in range(downs - 1)]
        total = functools.reduce(jnp.add, means)
        spreads = functools.reduce(jnp.add, [ms[j, 1]] + [mr[d, j, 1] for d in range(downs - 1)])
        mean = total * (1.0 / downs)
        between = functools.reduce(jnp.add, [(a - mean) * (a - mean) for a in means])
        variance = (spreads + between * Z) * (1.0 / (Z * downs))
        scale = lax.rsqrt(variance + 0.0001)
        for r, x in enumerate((j, X - 1 - j)):
            for y in range(Y):
                k = r * Y + y
                st[y, x] = (u[STEPS, y + 1, x + 1] - mean[k : k + 1]) * scale[k : k + 1]
        for x in (j, X - 1 - j):
            save_std(x).start()

    for t in range(STEPS):

        def step(j, carry, t=t):
            advance(t, j)
            if t + 1 < STEPS:
                for side in (0, 1):
                    down(side, t + 1, j).start()

                @pl.when(j == 0)
                def _():
                    for side in (0, 1):
                        east(side, t + 1).start()

                n = t * pairs + j + AHEAD
                south_pair(n // pairs, n % pairs)
            else:
                for d in range(1, downs):
                    moments(d, j).start()
                for x in (j, X - 1 - j):
                    save_line(STEPS, 0, x).start()

                @pl.when(j + AHEAD < pairs)
                def _():
                    south_pair(t, j + AHEAD)

                @pl.when(j >= LAG)
                def _():
                    finish(j - LAG)

            return carry

        lax.fori_loop(0, pairs, step, 0)

    def tail(j, carry):
        finish(j)
        return carry

    lax.fori_loop(pairs - LAG, pairs, tail, 0)

    def drain(x, carry):
        save_line(STEPS, 0, x).wait()
        save_std(x).wait()
        for side in (0, 1):
            for t in range(STEPS):
                south(side, t, x).wait_send()
        return carry

    lax.fori_loop(0, X, drain, 0)

    def drain_pairs(j, carry):
        for side in (0, 1):
            for t in range(STEPS):
                down(side, t, j).wait_send()
        for d in range(1, downs):
            moments(d, j).wait_send()
        return carry

    lax.fori_loop(0, pairs, drain_pairs, 0)
    for side in (0, 1):
        for t in range(STEPS):
            east(side, t).wait_send()


def body(tracer, mobility, source):
    sizes = tuple(lax.axis_size(a) for a in ("south", "east", "down"))
    Y, X, Z, L = tracer.shape
    downs, pairs = sizes[2], X // 2
    f32 = jnp.float32
    dma = pltpu.SemaphoreType.DMA
    shape = jax.ShapeDtypeStruct(tracer.shape, f32)
    anywhere = pl.BlockSpec(memory_space=pl.ANY)
    return pl.pallas_call(
        functools.partial(kernel, sizes),
        out_shape=(shape, shape),
        in_specs=[anywhere] * 3,
        out_specs=(anywhere, anywhere),
        scratch_shapes=[
            pltpu.VMEM((STEPS + 1, Y + 2, X + 2, Z, L), f32),
            pltpu.VMEM((Y, X, Z, L), f32),
            pltpu.VMEM((Y, X, Z, L), f32),
            pltpu.VMEM((Y, X, Z, L), f32),
            pltpu.VMEM((STEPS, 2, pairs, 2 * Y, L), f32),
            pltpu.VMEM((STEPS, 2, pairs, 2 * Y, L), f32),
            pltpu.VMEM((pairs, 2, 2 * Y, L), f32),
            pltpu.VMEM((downs - 1, pairs, 2, 2 * Y, L), f32),
            dma((Y + 2,)),
            dma((2, X)),
            dma((2, STEPS, X)),
            dma((2, STEPS, X)),
            dma((2, STEPS)),
            dma((2, STEPS)),
            dma((2, STEPS, pairs)),
            dma((2, STEPS, pairs)),
            dma((downs - 1, pairs)),
            dma((downs - 1, pairs)),
        ],
        compiler_params=pltpu.CompilerParams(
            collective_id=0, has_side_effects=True, vmem_limit_bytes=60 * 1024 * 1024
        ),
    )(tracer, mobility, source)


def solution(mesh):
    spec = P(("trial", "south"), "east", "down", None)
    return jax.shard_map(
        body, mesh=mesh, in_specs=(spec,) * 3, out_specs=(spec,) * 2, check_vma=False
    )
```

```python
import functools

import jax
import jax.numpy as jnp
from jax import lax
from jax.experimental import pallas as pl
from jax.experimental.pallas import tpu as pltpu
from jax.sharding import PartitionSpec as P

STEPS = 3
AHEAD = 4
LAG = 3
MESH = pl.DeviceIdType.MESH


def kernel(
    sizes,
    tr, mo, so,
    st, end,
    u, m, s, zs, zr, ms, mr,
    in_sem, s_send, s_recv, e_send, e_recv, z_send, z_recv, m_send, m_recv,
):
    souths, easts, downs = sizes
    Y, X, Z, L = tr.shape
    pairs = X // 2
    rows = 2 * Y
    at = {name: lax.axis_index(name) for name in ("south", "east", "down")}

    def peer(name, count, shift):
        return {name: lax.rem(at[name] + shift + count, count)}

    def south(side, t, j, x):
        return pltpu.make_async_remote_copy(
            src_ref=u.at[t, Y if side else 1, x + 1],
            dst_ref=u.at[t, 0 if side else Y + 1, x + 1],
            send_sem=s_send,
            recv_sem=s_recv.at[t, j],
            device_id=peer("south", souths, 1 if side else -1),
            device_id_type=MESH,
        )

    def east(side, t):
        return pltpu.make_async_remote_copy(
            src_ref=u.at[t, pl.ds(1, Y), X if side else 1],
            dst_ref=u.at[t, pl.ds(1, Y), 0 if side else X + 1],
            send_sem=e_send,
            recv_sem=e_recv.at[t],
            device_id=peer("east", easts, 1 if side else -1),
            device_id_type=MESH,
        )

    def down(side, t, j):
        return pltpu.make_async_remote_copy(
            src_ref=zs.at[t, side, j],
            dst_ref=zr.at[t, side, j],
            send_sem=z_send,
            recv_sem=z_recv.at[t, j],
            device_id=peer("down", downs, 1 if side else -1),
            device_id_type=MESH,
        )

    def moments(d, j):
        return pltpu.make_async_remote_copy(
            src_ref=ms.at[j],
            dst_ref=mr.at[d - 1, j],
            send_sem=m_send,
            recv_sem=m_recv.at[j],
            device_id=peer("down", downs, d),
            device_id_type=MESH,
        )

    def south_pair(t, j):
        for side in (0, 1):
            for x in (j, X - 1 - j):
                south(side, t, j, x).start()

    def arrived(ref, sem):
        everything = pltpu.make_async_remote_copy(
            src_ref=ref, dst_ref=ref, send_sem=sem, recv_sem=sem,
            device_id=peer("south", souths, 1), device_id_type=MESH,
        )
        everything.wait_recv()

    loads = [
        pltpu.make_async_copy(tr.at[y], u.at[0, y + 1, pl.ds(1, X)], in_sem.at[y])
        for y in range(Y)
    ]
    for y in [0, Y - 1] + list(range(1, Y - 1)):
        loads[y].start()
    others = [
        pltpu.make_async_copy(mo, m, in_sem.at[Y]),
        pltpu.make_async_copy(so, s, in_sem.at[Y + 1]),
    ]
    for copy in others:
        copy.start()

    barrier = pltpu.get_barrier_semaphore()
    greet = [peer("south", souths, d) for d in (-1, 1)]
    greet += [peer("east", easts, d) for d in (-1, 1)]
    greet += [peer("down", downs, d) for d in range(1, downs)]
    for who in greet:
        pl.semaphore_signal(barrier, inc=1, device_id=who, device_id_type=MESH)
    pl.semaphore_wait(barrier, len(greet))

    for copy in loads:
        copy.wait()

    def first_faces(j, carry):
        for r, x in enumerate((j, X - 1 - j)):
            for y in range(Y):
                zs[0, 0, j, pl.ds(r * Y + y, 1), :] = u[0, y + 1, x + 1, pl.ds(0, 1), :]
                zs[0, 1, j, pl.ds(r * Y + y, 1), :] = u[0, y + 1, x + 1, pl.ds(Z - 1, 1), :]
        return carry

    lax.fori_loop(0, pairs, first_faces, 0)
    south_pair(0, 0)
    for side in (0, 1):
        east(side, 0).start()

    def first_down(j, carry):
        for side in (0, 1):
            down(side, 0, j).start()
        return carry

    lax.fori_loop(0, pairs, first_down, 0)
    for j in range(1, AHEAD):
        south_pair(0, j)
    for copy in others:
        copy.wait()

    level = lax.broadcasted_iota(jnp.int32, (Z, L), 0)
    top, bottom = level == 0, level == Z - 1

    def advance(t, j):
        arrived(zr.at[t, :, j], z_recv.at[t, j])
        arrived(u.at[t, 0, pl.ds(0, 4)], s_recv.at[t, j])

        @pl.when(j == 0)
        def _():
            arrived(u.at[t, pl.ds(1, Y), pl.ds(0, 2)], e_recv.at[t])

        for r, x in enumerate((j, X - 1 - j)):
            for y in range(Y):
                at_row = pl.ds(r * Y + y, 1)
                middle = u[t, y + 1, x + 1]
                before = jnp.where(top, zr[t, 1, j, at_row, :], pltpu.roll(middle, 1, 0))
                after = jnp.where(bottom, zr[t, 0, j, at_row, :], pltpu.roll(middle, Z - 1, 0))
                spread = u[t, y, x + 1] + u[t, y + 2, x + 1] + u[t, y + 1, x] + u[t, y + 1, x + 2]
                spread = spread + before + after - 6.0 * middle
                value = middle + m[y, x] * spread + s[y, x]
                if t + 1 < STEPS:
                    u[t + 1, y + 1, x + 1] = value
                    zs[t + 1, 0, j, at_row, :] = value[:1]
                    zs[t + 1, 1, j, at_row, :] = value[Z - 1 :]
                else:
                    end[y, x] = value
                    mean = jnp.sum(value, axis=0, keepdims=True) * (1.0 / Z)
                    off = value - mean
                    ms[j, 0, at_row, :] = mean
                    ms[j, 1, at_row, :] = jnp.sum(off * off, axis=0, keepdims=True)

    def finish(j):
        arrived(mr.at[:, j], m_recv.at[j])
        means = [ms[j, 0]] + [mr[d, j, 0] for d in range(downs - 1)]
        total = functools.reduce(jnp.add, means)
        spreads = functools.reduce(jnp.add, [ms[j, 1]] + [mr[d, j, 1] for d in range(downs - 1)])
        mean = total * (1.0 / downs)
        between = functools.reduce(jnp.add, [(a - mean) * (a - mean) for a in means])
        variance = (spreads + between * Z) * (1.0 / (Z * downs))
        scale = lax.rsqrt(variance + 0.0001)
        for r, x in enumerate((j, X - 1 - j)):
            for y in range(Y):
                k = r * Y + y
                st[y, x] = (end[y, x] - mean[k : k + 1]) * scale[k : k + 1]

    for t in range(STEPS):

        def step(j, carry, t=t):
            advance(t, j)
            if t + 1 < STEPS:
                for side in (0, 1):
                    down(side, t + 1, j).start()

                @pl.when(j == 0)
                def _():
                    for side in (0, 1):
                        east(side, t + 1).start()

                n = t * pairs + j + AHEAD
                south_pair(n // pairs, n % pairs)
            else:
                for d in range(1, downs):
                    moments(d, j).start()

                @pl.when(j + AHEAD < pairs)
                def _():
                    south_pair(t, j + AHEAD)

                @pl.when(j >= LAG)
                def _():
                    finish(j - LAG)

            return carry

        lax.fori_loop(0, pairs, step, 0)

    def tail(j, carry):
        finish(j)
        return carry

    lax.fori_loop(pairs - LAG, pairs, tail, 0)

    arrived(u.at[:, pl.ds(0, 2), pl.ds(1, X)], s_send)
    arrived(u.at[:, pl.ds(0, 2), pl.ds(0, Y)], e_send)
    arrived(zs, z_send)
    arrived(mr, m_send)


def put_out(std, end, std_o, end_o, sem):
    copies = [
        pltpu.make_async_copy(std, std_o, sem.at[0]),
        pltpu.make_async_copy(end, end_o, sem.at[1]),
    ]
    for copy in copies:
        copy.start()
    for copy in copies:
        copy.wait()


def body(tracer, mobility, source):
    sizes = tuple(lax.axis_size(a) for a in ("south", "east", "down"))
    Y, X, Z, L = tracer.shape
    downs, pairs = sizes[2], X // 2
    f32 = jnp.float32
    dma = pltpu.SemaphoreType.DMA
    result = pltpu.VMEM(tracer.shape, f32)
    anywhere = pl.BlockSpec(memory_space=pl.ANY)
    onchip = pl.BlockSpec(memory_space=pltpu.VMEM)
    standardized, final = pl.pallas_call(
        functools.partial(kernel, sizes),
        out_shape=(result, result),
        in_specs=[anywhere] * 3,
        out_specs=(onchip, onchip),
        scratch_shapes=[
            pltpu.VMEM((STEPS, Y + 2, X + 2, Z, L), f32),
            pltpu.VMEM((Y, X, Z, L), f32),
            pltpu.VMEM((Y, X, Z, L), f32),
            pltpu.VMEM((STEPS, 2, pairs, 2 * Y, L), f32),
            pltpu.VMEM((STEPS, 2, pairs, 2 * Y, L), f32),
            pltpu.VMEM((pairs, 2, 2 * Y, L), f32),
            pltpu.VMEM((downs - 1, pairs, 2, 2 * Y, L), f32),
            dma((Y + 2,)),
            dma,
            dma((STEPS, pairs)),
            dma,
            dma((STEPS,)),
            dma,
            dma((STEPS, pairs)),
            dma,
            dma((pairs,)),
        ],
        compiler_params=pltpu.CompilerParams(
            collective_id=0, has_side_effects=True, vmem_limit_bytes=53 * 1024 * 1024
        ),
    )(tracer, mobility, source)
    shape = jax.ShapeDtypeStruct(tracer.shape, f32)
    return pl.pallas_call(
        put_out,
        out_shape=(shape, shape),
        in_specs=[onchip] * 2,
        out_specs=(anywhere, anywhere),
        scratch_shapes=[dma((2,))],
        compiler_params=pltpu.CompilerParams(vmem_limit_bytes=1024 * 1024),
    )(standardized, final)


def solution(mesh):
    spec = P(("trial", "south"), "east", "down", None)
    return jax.shard_map(
        body, mesh=mesh, in_specs=(spec,) * 3, out_specs=(spec,) * 2, check_vma=False
    )
```

```python
import functools

import jax
import jax.numpy as jnp
from jax import lax
from jax.experimental import pallas as pl
from jax.experimental.pallas import tpu as pltpu
from jax.sharding import PartitionSpec as P

STEPS = 3
FIRST = 3
AHEAD = 6
LAG = 3
MESH = pl.DeviceIdType.MESH


def kernel(
    sizes,
    tr, mo, so,
    st, end,
    u, m, s, zs, zr, ms, mr,
    known, in_sem, s_send, s_recv, e_send, e_recv, z_send, z_recv, m_send, m_recv,
):
    trials, souths, easts, downs = sizes
    Y, X, Z, L = tr.shape
    pairs = X // 2
    rows = 2 * Y
    at = {name: lax.axis_index(name) for name in ("trial", "south", "east", "down")}

    def peer(name, count, shift):
        return {name: lax.rem(at[name] + shift + count, count)}

    def away(dy=0, dz=0):
        y = lax.rem(at["down"] % 2 * 2 + at["south"] // 2 + dy + 4, 4)
        z = lax.rem(at["down"] // 2 * trials + at["trial"] + dz + 2 * trials, 2 * trials)
        return {
            "trial": z % trials,
            "south": y % 2 * 2 + at["south"] % 2,
            "down": z // trials * 2 + y // 2,
        }

    def south(side, t, j, x):
        return pltpu.make_async_remote_copy(
            src_ref=u.at[t, Y if side else 1, x + 1],
            dst_ref=u.at[t, 0 if side else Y + 1, x + 1],
            send_sem=s_send,
            recv_sem=s_recv.at[t, j],
            device_id=peer("south", souths, 1 if side else -1),
            device_id_type=MESH,
        )

    def east(side, t):
        return pltpu.make_async_remote_copy(
            src_ref=u.at[t, pl.ds(1, Y), X if side else 1],
            dst_ref=u.at[t, pl.ds(1, Y), 0 if side else X + 1],
            send_sem=e_send,
            recv_sem=e_recv.at[t],
            device_id=peer("east", easts, 1 if side else -1),
            device_id_type=MESH,
        )

    def down(side, t, j):
        return pltpu.make_async_remote_copy(
            src_ref=zs.at[t, side, j],
            dst_ref=zr.at[t, side, j],
            send_sem=z_send,
            recv_sem=z_recv.at[t, j],
            device_id=peer("down", downs, 1 if side else -1),
            device_id_type=MESH,
        )

    def moments(d, j):
        return pltpu.make_async_remote_copy(
            src_ref=ms.at[j],
            dst_ref=mr.at[d - 1, j],
            send_sem=m_send,
            recv_sem=m_recv.at[j],
            device_id=peer("down", downs, d),
            device_id_type=MESH,
        )

    def south_pair(t, j):
        for side in (0, 1):
            for x in (j, X - 1 - j):
                south(side, t, j, x).start()

    def arrived(ref, sem):
        everything = pltpu.make_async_remote_copy(
            src_ref=ref, dst_ref=ref, send_sem=sem, recv_sem=sem,
            device_id=peer("south", souths, 1), device_id_type=MESH,
        )
        everything.wait_recv()

    loads = [
        pltpu.make_async_copy(tr.at[y], u.at[0, y + 1, pl.ds(1, X)], in_sem.at[y])
        for y in range(Y)
    ]
    for y in [0, Y - 1] + list(range(1, Y - 1)):
        loads[y].start()
    others = [
        pltpu.make_async_copy(mo, m, in_sem.at[Y]),
        pltpu.make_async_copy(so, s, in_sem.at[Y + 1]),
    ]
    for copy in others:
        copy.start()

    barrier = pltpu.get_barrier_semaphore()
    near = [peer("south", souths, d) for d in (-1, 1)]
    near += [peer("east", easts, d) for d in (-1, 1)]
    near += [away(dy=d) for d in (-1, 1)] + [away(dz=d) for d in (-1, 1)]
    for who in near:
        pl.semaphore_signal(barrier, inc=1, device_id=who, device_id_type=MESH)
    pl.semaphore_wait(barrier, len(near))

    loads[0].wait()
    loads[Y - 1].wait()
    for j in range(FIRST):
        south_pair(0, j)
    for y in range(1, Y - 1):
        loads[y].wait()
    for side in (0, 1):
        east(side, 0).start()

    def first_faces(j, carry):
        for r, x in enumerate((j, X - 1 - j)):
            for y in range(Y):
                zs[0, 0, j, pl.ds(r * Y + y, 1), :] = u[0, y + 1, x + 1, pl.ds(0, 1), :]
                zs[0, 1, j, pl.ds(r * Y + y, 1), :] = u[0, y + 1, x + 1, pl.ds(Z - 1, 1), :]
        return carry

    lax.fori_loop(0, pairs, first_faces, 0)

    rounds = ([away(dz=-1), away(dz=1)], [away(dz=-2)], [away(dy=-1)], [away(dy=-1)])
    for i, to in enumerate(rounds):
        for who in to:
            pl.semaphore_signal(known.at[i], inc=1, device_id=who, device_id_type=MESH)
        pl.semaphore_wait(known.at[i], len(to))

    def first_down(j, carry):
        for side in (0, 1):
            down(side, 0, j).start()
        return carry

    lax.fori_loop(0, pairs, first_down, 0)
    for j in range(FIRST, AHEAD):
        south_pair(0, j)
    for copy in others:
        copy.wait()

    level = lax.broadcasted_iota(jnp.int32, (Z, L), 0)
    top, bottom = level == 0, level == Z - 1

    def advance(t, j):
        arrived(zr.at[t, :, j], z_recv.at[t, j])
        arrived(u.at[t, 0, pl.ds(0, 4)], s_recv.at[t, j])

        @pl.when(j == 0)
        def _():
            arrived(u.at[t, pl.ds(1, Y), pl.ds(0, 2)], e_recv.at[t])

        for r, x in enumerate((j, X - 1 - j)):
            for y in range(Y):
                at_row = pl.ds(r * Y + y, 1)
                middle = u[t, y + 1, x + 1]
                before = jnp.where(top, zr[t, 1, j, at_row, :], pltpu.roll(middle, 1, 0))
                after = jnp.where(bottom, zr[t, 0, j, at_row, :], pltpu.roll(middle, Z - 1, 0))
                spread = u[t, y, x + 1] + u[t, y + 2, x + 1] + u[t, y + 1, x] + u[t, y + 1, x + 2]
                spread = spread + before + after - 6.0 * middle
                value = middle + m[y, x] * spread + s[y, x]
                if t + 1 < STEPS:
                    u[t + 1, y + 1, x + 1] = value
                    zs[t + 1, 0, j, at_row, :] = value[:1]
                    zs[t + 1, 1, j, at_row, :] = value[Z - 1 :]
                else:
                    end[y, x] = value
                    mean = jnp.sum(value, axis=0, keepdims=True) * (1.0 / Z)
                    off = value - mean
                    ms[j, 0, at_row, :] = mean
                    ms[j, 1, at_row, :] = jnp.sum(off * off, axis=0, keepdims=True)

    def finish(j):
        arrived(mr.at[:, j], m_recv.at[j])
        means = [ms[j, 0]] + [mr[d, j, 0] for d in range(downs - 1)]
        total = functools.reduce(jnp.add, means)
        spreads = functools.reduce(jnp.add, [ms[j, 1]] + [mr[d, j, 1] for d in range(downs - 1)])
        mean = total * (1.0 / downs)
        between = functools.reduce(jnp.add, [(a - mean) * (a - mean) for a in means])
        variance = (spreads + between * Z) * (1.0 / (Z * downs))
        scale = lax.rsqrt(variance + 0.0001)
        for r, x in enumerate((j, X - 1 - j)):
            for y in range(Y):
                k = r * Y + y
                st[y, x] = (end[y, x] - mean[k : k + 1]) * scale[k : k + 1]

    for t in range(STEPS):

        def step(j, carry, t=t):
            advance(t, j)
            if t + 1 < STEPS:
                for side in (0, 1):
                    down(side, t + 1, j).start()

                @pl.when(j == 0)
                def _():
                    for side in (0, 1):
                        east(side, t + 1).start()

                n = t * pairs + j + AHEAD
                south_pair(n // pairs, n % pairs)
            else:
                for d in range(1, downs):
                    moments(d, j).start()

                @pl.when(j + AHEAD < pairs)
                def _():
                    south_pair(t, j + AHEAD)

                @pl.when(j >= LAG)
                def _():
                    finish(j - LAG)

            return carry

        lax.fori_loop(0, pairs, step, 0)

    def tail(j, carry):
        finish(j)
        return carry

    lax.fori_loop(pairs - LAG, pairs, tail, 0)

    arrived(u.at[:, pl.ds(0, 2), pl.ds(1, X)], s_send)
    arrived(u.at[:, pl.ds(0, 2), pl.ds(0, Y)], e_send)
    arrived(zs, z_send)
    arrived(mr, m_send)


def put_out(std, end, std_o, end_o, sem):
    copies = [
        pltpu.make_async_copy(std, std_o, sem.at[0]),
        pltpu.make_async_copy(end, end_o, sem.at[1]),
    ]
    for copy in copies:
        copy.start()
    for copy in copies:
        copy.wait()


def body(tracer, mobility, source):
    sizes = tuple(lax.axis_size(a) for a in ("trial", "south", "east", "down"))
    Y, X, Z, L = tracer.shape
    downs, pairs = sizes[3], X // 2
    f32 = jnp.float32
    dma = pltpu.SemaphoreType.DMA
    result = pltpu.VMEM(tracer.shape, f32)
    anywhere = pl.BlockSpec(memory_space=pl.ANY)
    onchip = pl.BlockSpec(memory_space=pltpu.VMEM)
    standardized, final = pl.pallas_call(
        functools.partial(kernel, sizes),
        out_shape=(result, result),
        in_specs=[anywhere] * 3,
        out_specs=(onchip, onchip),
        scratch_shapes=[
            pltpu.VMEM((STEPS, Y + 2, X + 2, Z, L), f32),
            pltpu.VMEM((Y, X, Z, L), f32),
            pltpu.VMEM((Y, X, Z, L), f32),
            pltpu.VMEM((STEPS, 2, pairs, 2 * Y, L), f32),
            pltpu.VMEM((STEPS, 2, pairs, 2 * Y, L), f32),
            pltpu.VMEM((pairs, 2, 2 * Y, L), f32),
            pltpu.VMEM((downs - 1, pairs, 2, 2 * Y, L), f32),
            pltpu.SemaphoreType.REGULAR((4,)),
            dma((Y + 2,)),
            dma,
            dma((STEPS, pairs)),
            dma,
            dma((STEPS,)),
            dma,
            dma((STEPS, pairs)),
            dma,
            dma((pairs,)),
        ],
        compiler_params=pltpu.CompilerParams(
            collective_id=0, has_side_effects=True, vmem_limit_bytes=53 * 1024 * 1024
        ),
    )(tracer, mobility, source)
    shape = jax.ShapeDtypeStruct(tracer.shape, f32)
    return pl.pallas_call(
        put_out,
        out_shape=(shape, shape),
        in_specs=[onchip] * 2,
        out_specs=(anywhere, anywhere),
        scratch_shapes=[dma((2,))],
        compiler_params=pltpu.CompilerParams(vmem_limit_bytes=1024 * 1024),
    )(standardized, final)


def solution(mesh):
    spec = P(("trial", "south"), "east", "down", None)
    return jax.shard_map(
        body, mesh=mesh, in_specs=(spec,) * 3, out_specs=(spec,) * 2, check_vma=False
    )
```

```python
import functools

import jax
import jax.numpy as jnp
from jax import lax
from jax.experimental import pallas as pl
from jax.experimental.pallas import tpu as pltpu
from jax.sharding import PartitionSpec as P

STEPS = 3
FIRST = 3
AHEAD = 6
DIRECT = 2
MESH = pl.DeviceIdType.MESH


def kernel(
    sizes,
    tr, mo, so,
    st, end,
    u, m, s, zs, zr, ms, mz, mc, my, mr,
    known, in_sem, s_send, s_recv, e_send, e_recv, z_send, z_recv, m_send, m_recv,
):
    trials, souths, easts, downs = sizes
    Y, X, Z, L = tr.shape
    pairs = X // 2
    rows = 2 * Y
    at = {name: lax.axis_index(name) for name in ("trial", "south", "east", "down")}

    across = 2
    beside = 1 + at["down"] % 2 * 2

    def peer(name, count, shift):
        return {name: lax.rem(at[name] + shift + count, count)}

    def away(dy=0, dz=0):
        y = lax.rem(at["down"] % 2 * 2 + at["south"] // 2 + dy + 4, 4)
        z = lax.rem(at["down"] // 2 * trials + at["trial"] + dz + 2 * trials, 2 * trials)
        return {
            "trial": z % trials,
            "south": y % 2 * 2 + at["south"] % 2,
            "down": z // trials * 2 + y // 2,
        }

    def south(side, t, j, x):
        return pltpu.make_async_remote_copy(
            src_ref=u.at[t, Y if side else 1, x + 1],
            dst_ref=u.at[t, 0 if side else Y + 1, x + 1],
            send_sem=s_send,
            recv_sem=s_recv.at[t, j],
            device_id=peer("south", souths, 1 if side else -1),
            device_id_type=MESH,
        )

    def east(side, t):
        return pltpu.make_async_remote_copy(
            src_ref=u.at[t, pl.ds(1, Y), X if side else 1],
            dst_ref=u.at[t, pl.ds(1, Y), 0 if side else X + 1],
            send_sem=e_send,
            recv_sem=e_recv.at[t],
            device_id=peer("east", easts, 1 if side else -1),
            device_id_type=MESH,
        )

    def down(side, t, j):
        return pltpu.make_async_remote_copy(
            src_ref=zs.at[t, side, j],
            dst_ref=zr.at[t, side, j],
            send_sem=z_send,
            recv_sem=z_recv.at[t, j],
            device_id=peer("down", downs, 1 if side else -1),
            device_id_type=MESH,
        )

    merged = pairs - DIRECT

    def share(src, dst, d, i):
        return pltpu.make_async_remote_copy(
            src_ref=src,
            dst_ref=dst,
            send_sem=m_send.at[i],
            recv_sem=m_recv.at[i],
            device_id=peer("down", downs, d),
            device_id_type=MESH,
        )

    def south_pair(t, j):
        for side in (0, 1):
            for x in (j, X - 1 - j):
                south(side, t, j, x).start()

    def arrived(ref, sem):
        everything = pltpu.make_async_remote_copy(
            src_ref=ref, dst_ref=ref, send_sem=sem, recv_sem=sem,
            device_id=peer("south", souths, 1), device_id_type=MESH,
        )
        everything.wait_recv()

    loads = [
        pltpu.make_async_copy(tr.at[y], u.at[0, y + 1, pl.ds(1, X)], in_sem.at[y])
        for y in range(Y)
    ]
    for y in [0, Y - 1] + list(range(1, Y - 1)):
        loads[y].start()
    others = [
        pltpu.make_async_copy(mo, m, in_sem.at[Y]),
        pltpu.make_async_copy(so, s, in_sem.at[Y + 1]),
    ]
    for copy in others:
        copy.start()

    barrier = pltpu.get_barrier_semaphore()
    near = [peer("south", souths, d) for d in (-1, 1)]
    near += [peer("east", easts, d) for d in (-1, 1)]
    near += [away(dy=d) for d in (-1, 1)] + [away(dz=d) for d in (-1, 1)]
    for who in near:
        pl.semaphore_signal(barrier, inc=1, device_id=who, device_id_type=MESH)
    pl.semaphore_wait(barrier, len(near))

    loads[0].wait()
    loads[Y - 1].wait()
    for j in range(FIRST):
        south_pair(0, j)
    for y in range(1, Y - 1):
        loads[y].wait()
    for side in (0, 1):
        east(side, 0).start()

    def first_faces(j, carry):
        for r, x in enumerate((j, X - 1 - j)):
            for y in range(Y):
                zs[0, 0, j, pl.ds(r * Y + y, 1), :] = u[0, y + 1, x + 1, pl.ds(0, 1), :]
                zs[0, 1, j, pl.ds(r * Y + y, 1), :] = u[0, y + 1, x + 1, pl.ds(Z - 1, 1), :]
        return carry

    lax.fori_loop(0, pairs, first_faces, 0)

    rounds = ([away(dz=-1), away(dz=1)], [away(dz=-2)], [away(dy=-1)], [away(dy=-1)])
    for i, to in enumerate(rounds):
        for who in to:
            pl.semaphore_signal(known.at[i], inc=1, device_id=who, device_id_type=MESH)
        pl.semaphore_wait(known.at[i], len(to))

    def first_down(j, carry):
        for side in (0, 1):
            down(side, 0, j).start()
        return carry

    lax.fori_loop(0, pairs, first_down, 0)
    for j in range(FIRST, AHEAD):
        south_pair(0, j)
    for copy in others:
        copy.wait()

    level = lax.broadcasted_iota(jnp.int32, (Z, L), 0)
    top, bottom = level == 0, level == Z - 1

    def advance(t, j):
        arrived(zr.at[t, :, j], z_recv.at[t, j])
        arrived(u.at[t, 0, pl.ds(0, 4)], s_recv.at[t, j])

        @pl.when(j == 0)
        def _():
            arrived(u.at[t, pl.ds(1, Y), pl.ds(0, 2)], e_recv.at[t])

        for r, x in enumerate((j, X - 1 - j)):
            for y in range(Y):
                at_row = pl.ds(r * Y + y, 1)
                middle = u[t, y + 1, x + 1]
                before = jnp.where(top, zr[t, 1, j, at_row, :], pltpu.roll(middle, 1, 0))
                after = jnp.where(bottom, zr[t, 0, j, at_row, :], pltpu.roll(middle, Z - 1, 0))
                spread = u[t, y, x + 1] + u[t, y + 2, x + 1] + u[t, y + 1, x] + u[t, y + 1, x + 2]
                spread = spread + before + after - 6.0 * middle
                value = middle + m[y, x] * spread + s[y, x]
                if t + 1 < STEPS:
                    u[t + 1, y + 1, x + 1] = value
                    zs[t + 1, 0, j, at_row, :] = value[:1]
                    zs[t + 1, 1, j, at_row, :] = value[Z - 1 :]
                else:
                    end[y, x] = value
                    mean = jnp.sum(value, axis=0, keepdims=True) * (1.0 / Z)
                    off = value - mean
                    ms[j, 0, at_row, :] = mean
                    ms[j, 1, at_row, :] = jnp.sum(off * off, axis=0, keepdims=True)

    def finish(j, mean, spreads):
        scale = lax.rsqrt(spreads * (1.0 / (Z * downs)) + 0.0001)
        for r, x in enumerate((j, X - 1 - j)):
            for y in range(Y):
                k = r * Y + y
                st[y, x] = (end[y, x] - mean[k : k + 1]) * scale[k : k + 1]

    for t in range(STEPS):

        def step(j, carry, t=t):
            advance(t, j)
            if t + 1 < STEPS:
                for side in (0, 1):
                    down(side, t + 1, j).start()

                @pl.when(j == 0)
                def _():
                    for side in (0, 1):
                        east(side, t + 1).start()

                n = t * pairs + j + AHEAD
                south_pair(n // pairs, n % pairs)
            else:

                @pl.when(j < merged)
                def _():
                    share(ms.at[j], mz.at[j], across, 0).start()

                @pl.when(j >= merged)
                def _():
                    k = j - merged
                    for d in range(1, downs):
                        share(ms.at[j], mr.at[k, d - 1], d, 2 + k).start()

                @pl.when(j + AHEAD < pairs)
                def _():
                    south_pair(t, j + AHEAD)

            return carry

        lax.fori_loop(0, pairs, step, 0)

    arrived(mz, m_recv.at[0])

    def merge(j, carry):
        gap = ms[j, 0] - mz[j, 0]
        mc[j, 0] = (ms[j, 0] + mz[j, 0]) * 0.5
        mc[j, 1] = ms[j, 1] + mz[j, 1] + gap * gap * (0.5 * Z)
        return carry

    lax.fori_loop(0, merged, merge, 0)
    share(mc, my, beside, 1).start()
    arrived(my, m_recv.at[1])

    def finish_merged(j, carry):
        gap = mc[j, 0] - my[j, 0]
        finish(j, (mc[j, 0] + my[j, 0]) * 0.5, mc[j, 1] + my[j, 1] + gap * gap * (1.0 * Z))
        return carry

    lax.fori_loop(0, merged, finish_merged, 0)

    def finish_direct(k, carry):
        j = merged + k
        arrived(mr.at[k], m_recv.at[2 + k])
        means = [ms[j, 0]] + [mr[k, d, 0] for d in range(downs - 1)]
        mean = functools.reduce(jnp.add, means) * (1.0 / downs)
        spreads = functools.reduce(jnp.add, [ms[j, 1]] + [mr[k, d, 1] for d in range(downs - 1)])
        between = functools.reduce(jnp.add, [(a - mean) * (a - mean) for a in means])
        finish(j, mean, spreads + between * Z)
        return carry

    lax.fori_loop(0, DIRECT, finish_direct, 0)

    arrived(u.at[:, pl.ds(0, 2), pl.ds(1, X)], s_send)
    arrived(u.at[:, pl.ds(0, 2), pl.ds(0, Y)], e_send)
    arrived(zs, z_send)
    for i, ref in enumerate([mz, my] + [mr.at[k] for k in range(DIRECT)]):
        arrived(ref, m_send.at[i])


def put_out(std, end, std_o, end_o, sem):
    copies = []
    for y in range(std.shape[0]):
        copies.append(pltpu.make_async_copy(end.at[y], end_o.at[y], sem.at[0, y]))
        copies.append(pltpu.make_async_copy(std.at[y], std_o.at[y], sem.at[1, y]))
    for copy in copies:
        copy.start()
    for copy in copies:
        copy.wait()


def body(tracer, mobility, source):
    sizes = tuple(lax.axis_size(a) for a in ("trial", "south", "east", "down"))
    Y, X, Z, L = tracer.shape
    downs, pairs = sizes[3], X // 2
    f32 = jnp.float32
    dma = pltpu.SemaphoreType.DMA
    result = pltpu.VMEM(tracer.shape, f32)
    anywhere = pl.BlockSpec(memory_space=pl.ANY)
    onchip = pl.BlockSpec(memory_space=pltpu.VMEM)
    standardized, final = pl.pallas_call(
        functools.partial(kernel, sizes),
        out_shape=(result, result),
        in_specs=[anywhere] * 3,
        out_specs=(onchip, onchip),
        scratch_shapes=[
            pltpu.VMEM((STEPS, Y + 2, X + 2, Z, L), f32),
            pltpu.VMEM((Y, X, Z, L), f32),
            pltpu.VMEM((Y, X, Z, L), f32),
            pltpu.VMEM((STEPS, 2, pairs, 2 * Y, L), f32),
            pltpu.VMEM((STEPS, 2, pairs, 2 * Y, L), f32),
            pltpu.VMEM((pairs, 2, 2 * Y, L), f32),
            pltpu.VMEM((pairs - DIRECT, 2, 2 * Y, L), f32),
            pltpu.VMEM((pairs - DIRECT, 2, 2 * Y, L), f32),
            pltpu.VMEM((pairs - DIRECT, 2, 2 * Y, L), f32),
            pltpu.VMEM((DIRECT, downs - 1, 2, 2 * Y, L), f32),
            pltpu.SemaphoreType.REGULAR((4,)),
            dma((Y + 2,)),
            dma,
            dma((STEPS, pairs)),
            dma,
            dma((STEPS,)),
            dma,
            dma((STEPS, pairs)),
            dma((2 + DIRECT,)),
            dma((2 + DIRECT,)),
        ],
        compiler_params=pltpu.CompilerParams(
            collective_id=0, has_side_effects=True, vmem_limit_bytes=53 * 1024 * 1024
        ),
    )(tracer, mobility, source)
    shape = jax.ShapeDtypeStruct(tracer.shape, f32)
    return pl.pallas_call(
        put_out,
        out_shape=(shape, shape),
        in_specs=[onchip] * 2,
        out_specs=(anywhere, anywhere),
        scratch_shapes=[dma((2, Y))],
        compiler_params=pltpu.CompilerParams(vmem_limit_bytes=1024 * 1024),
    )(standardized, final)


def solution(mesh):
    spec = P(("trial", "south"), "east", "down", None)
    return jax.shard_map(
        body, mesh=mesh, in_specs=(spec,) * 3, out_specs=(spec,) * 2, check_vma=False
    )
```

```python
import functools

import jax
import jax.numpy as jnp
from jax import lax
from jax.experimental import pallas as pl
from jax.experimental.pallas import tpu as pltpu
from jax.sharding import PartitionSpec as P

STEPS = 3
FIRST = 3
AHEAD = 4
RELAY = 4
DIRECT = 2
MESH = pl.DeviceIdType.MESH


def kernel(
    sizes,
    tr, mo, so,
    st, end,
    u, m, s, zs, zr, rl, ms, mz, mc, my, mr,
    known, in_sem, s_send, s_recv, e_send, e_recv, z_send, z_recv, r_send, r_recv, m_send, m_recv,
):
    trials, souths, easts, downs = sizes
    Y, X, Z, L = tr.shape
    pairs = X // 2
    rows = 2 * Y
    at = {name: lax.axis_index(name) for name in ("trial", "south", "east", "down")}

    across = 2
    beside = 1 + at["down"] % 2 * 2

    def peer(name, count, shift):
        return {name: lax.rem(at[name] + shift + count, count)}

    def away(dy=0, dz=0):
        y = lax.rem(at["down"] % 2 * 2 + at["south"] // 2 + dy + 4, 4)
        z = lax.rem(at["down"] // 2 * trials + at["trial"] + dz + 2 * trials, 2 * trials)
        return {
            "trial": z % trials,
            "south": y % 2 * 2 + at["south"] % 2,
            "down": z // trials * 2 + y // 2,
        }

    def south(side, t, j, x):
        return pltpu.make_async_remote_copy(
            src_ref=u.at[t, Y if side else 1, x + 1],
            dst_ref=u.at[t, 0 if side else Y + 1, x + 1],
            send_sem=s_send,
            recv_sem=s_recv.at[t, j],
            device_id=peer("south", souths, 1 if side else -1),
            device_id_type=MESH,
        )

    def east(side, t):
        return pltpu.make_async_remote_copy(
            src_ref=u.at[t, pl.ds(1, Y), X if side else 1],
            dst_ref=u.at[t, pl.ds(1, Y), 0 if side else X + 1],
            send_sem=e_send,
            recv_sem=e_recv.at[t],
            device_id=peer("east", easts, 1 if side else -1),
            device_id_type=MESH,
        )

    def down(side, t, j):
        return pltpu.make_async_remote_copy(
            src_ref=zs.at[t, side, j],
            dst_ref=zr.at[t, side, j],
            send_sem=z_send,
            recv_sem=z_recv.at[t, j],
            device_id=peer("down", downs, 2 * side - 1),
            device_id_type=MESH,
        )

    early = at["down"] // 2 == 0
    inner = 1 - at["down"] % 2

    def hand(t, j):
        return pltpu.make_async_remote_copy(
            src_ref=zs.at[t, 1 - inner, j],
            dst_ref=rl.at[t - 1, j],
            send_sem=z_send,
            recv_sem=r_recv.at[t - 1, j],
            device_id=peer("down", downs, beside),
            device_id_type=MESH,
        )

    def forward(t, j):
        arrived(rl.at[t - 1, j], r_recv.at[t - 1, j])
        onward = pltpu.make_async_remote_copy(
            src_ref=rl.at[t - 1, j],
            dst_ref=zr.at[t, inner, j],
            send_sem=r_send,
            recv_sem=z_recv.at[t, j],
            device_id=peer("down", downs, across),
            device_id_type=MESH,
        )
        onward.start()

    def faces(t, j):
        @pl.when(early)
        def _():
            down(inner, t, j).start()
            hand(t, j).start()

        @pl.when(jnp.logical_not(early))
        def _():
            for side in (0, 1):
                down(side, t, j).start()

    merged = pairs - DIRECT

    def share(src, dst, d, i):
        return pltpu.make_async_remote_copy(
            src_ref=src,
            dst_ref=dst,
            send_sem=m_send.at[i],
            recv_sem=m_recv.at[i],
            device_id=peer("down", downs, d),
            device_id_type=MESH,
        )

    def south_pair(t, j):
        for side in (0, 1):
            for x in (j, X - 1 - j):
                south(side, t, j, x).start()

    def arrived(ref, sem):
        everything = pltpu.make_async_remote_copy(
            src_ref=ref, dst_ref=ref, send_sem=sem, recv_sem=sem,
            device_id=peer("south", souths, 1), device_id_type=MESH,
        )
        everything.wait_recv()

    loads = [
        pltpu.make_async_copy(tr.at[y], u.at[0, y + 1, pl.ds(1, X)], in_sem.at[y])
        for y in range(Y)
    ]
    for y in [0, Y - 1] + list(range(1, Y - 1)):
        loads[y].start()
    others = [
        pltpu.make_async_copy(mo, m, in_sem.at[Y]),
        pltpu.make_async_copy(so, s, in_sem.at[Y + 1]),
    ]
    for copy in others:
        copy.start()

    barrier = pltpu.get_barrier_semaphore()
    near = [peer("south", souths, d) for d in (-1, 1)]
    near += [peer("east", easts, d) for d in (-1, 1)]
    near += [away(dy=d) for d in (-1, 1)] + [away(dz=d) for d in (-1, 1)]
    for who in near:
        pl.semaphore_signal(barrier, inc=1, device_id=who, device_id_type=MESH)
    pl.semaphore_wait(barrier, len(near))

    loads[0].wait()
    loads[Y - 1].wait()
    for j in range(FIRST):
        south_pair(0, j)
    for y in range(1, Y - 1):
        loads[y].wait()
    for side in (0, 1):
        east(side, 0).start()

    def first_faces(j, carry):
        for r, x in enumerate((j, X - 1 - j)):
            for y in range(Y):
                zs[0, 0, j, pl.ds(r * Y + y, 1), :] = u[0, y + 1, x + 1, pl.ds(0, 1), :]
                zs[0, 1, j, pl.ds(r * Y + y, 1), :] = u[0, y + 1, x + 1, pl.ds(Z - 1, 1), :]
        return carry

    lax.fori_loop(0, pairs, first_faces, 0)

    rounds = ([away(dz=-1), away(dz=1)], [away(dz=-2)], [away(dy=-1)], [away(dy=-1)])
    for i, to in enumerate(rounds):
        for who in to:
            pl.semaphore_signal(known.at[i], inc=1, device_id=who, device_id_type=MESH)
        pl.semaphore_wait(known.at[i], len(to))

    def first_down(j, carry):
        for side in (0, 1):
            down(side, 0, j).start()
        return carry

    lax.fori_loop(0, pairs, first_down, 0)
    for j in range(FIRST, AHEAD):
        south_pair(0, j)
    for copy in others:
        copy.wait()

    level = lax.broadcasted_iota(jnp.int32, (Z, L), 0)
    top, bottom = level == 0, level == Z - 1

    def advance(t, j):
        arrived(zr.at[t, :, j], z_recv.at[t, j])
        arrived(u.at[t, 0, pl.ds(0, 4)], s_recv.at[t, j])

        @pl.when(j == 0)
        def _():
            arrived(u.at[t, pl.ds(1, Y), pl.ds(0, 2)], e_recv.at[t])

        for r, x in enumerate((j, X - 1 - j)):
            for y in range(Y):
                at_row = pl.ds(r * Y + y, 1)
                middle = u[t, y + 1, x + 1]
                before = jnp.where(top, zr[t, 1, j, at_row, :], pltpu.roll(middle, 1, 0))
                after = jnp.where(bottom, zr[t, 0, j, at_row, :], pltpu.roll(middle, Z - 1, 0))
                spread = u[t, y, x + 1] + u[t, y + 2, x + 1] + u[t, y + 1, x] + u[t, y + 1, x + 2]
                spread = spread + before + after - 6.0 * middle
                value = middle + m[y, x] * spread + s[y, x]
                if t + 1 < STEPS:
                    u[t + 1, y + 1, x + 1] = value
                    zs[t + 1, 0, j, at_row, :] = value[:1]
                    zs[t + 1, 1, j, at_row, :] = value[Z - 1 :]
                else:
                    end[y, x] = value
                    mean = jnp.sum(value, axis=0, keepdims=True) * (1.0 / Z)
                    off = value - mean
                    ms[j, 0, at_row, :] = mean
                    ms[j, 1, at_row, :] = jnp.sum(off * off, axis=0, keepdims=True)

    def finish(j, mean, spreads):
        scale = lax.rsqrt(spreads * (1.0 / (Z * downs)) + 0.0001)
        for r, x in enumerate((j, X - 1 - j)):
            for y in range(Y):
                k = r * Y + y
                st[y, x] = (end[y, x] - mean[k : k + 1]) * scale[k : k + 1]

    for t in range(STEPS):

        def step(j, carry, t=t):
            n = t * pairs + j - RELAY

            @pl.when(jnp.logical_and(early, jnp.logical_and(n >= 0, n < (STEPS - 1) * pairs)))
            def _():
                forward(n // pairs + 1, n % pairs)

            advance(t, j)
            if t + 1 < STEPS:
                faces(t + 1, j)

                @pl.when(j == 0)
                def _():
                    for side in (0, 1):
                        east(side, t + 1).start()

                n = t * pairs + j + AHEAD
                south_pair(n // pairs, n % pairs)
            else:

                @pl.when(j < merged)
                def _():
                    share(ms.at[j], mz.at[j], across, 0).start()

                @pl.when(j >= merged)
                def _():
                    k = j - merged
                    for d in range(1, downs):
                        share(ms.at[j], mr.at[k, d - 1], d, 2 + k).start()

                @pl.when(j + AHEAD < pairs)
                def _():
                    south_pair(t, j + AHEAD)

            return carry

        lax.fori_loop(0, pairs, step, 0)

    arrived(mz, m_recv.at[0])

    def merge(j, carry):
        gap = ms[j, 0] - mz[j, 0]
        mc[j, 0] = (ms[j, 0] + mz[j, 0]) * 0.5
        mc[j, 1] = ms[j, 1] + mz[j, 1] + gap * gap * (0.5 * Z)
        return carry

    lax.fori_loop(0, merged, merge, 0)
    share(mc, my, beside, 1).start()
    arrived(my, m_recv.at[1])

    def finish_merged(j, carry):
        gap = mc[j, 0] - my[j, 0]
        finish(j, (mc[j, 0] + my[j, 0]) * 0.5, mc[j, 1] + my[j, 1] + gap * gap * (1.0 * Z))
        return carry

    lax.fori_loop(0, merged, finish_merged, 0)

    def finish_direct(k, carry):
        j = merged + k
        arrived(mr.at[k], m_recv.at[2 + k])
        means = [ms[j, 0]] + [mr[k, d, 0] for d in range(downs - 1)]
        mean = functools.reduce(jnp.add, means) * (1.0 / downs)
        spreads = functools.reduce(jnp.add, [ms[j, 1]] + [mr[k, d, 1] for d in range(downs - 1)])
        between = functools.reduce(jnp.add, [(a - mean) * (a - mean) for a in means])
        finish(j, mean, spreads + between * Z)
        return carry

    lax.fori_loop(0, DIRECT, finish_direct, 0)

    arrived(u.at[:, pl.ds(0, 2), pl.ds(1, X)], s_send)
    arrived(u.at[:, pl.ds(0, 2), pl.ds(0, Y)], e_send)
    arrived(zs, z_send)

    @pl.when(early)
    def _():
        arrived(rl, r_send)

    for i, ref in enumerate([mz, my] + [mr.at[k] for k in range(DIRECT)]):
        arrived(ref, m_send.at[i])


def put_out(std, end, std_o, end_o, sem):
    copies = []
    for y in range(std.shape[0]):
        copies.append(pltpu.make_async_copy(end.at[y], end_o.at[y], sem.at[0, y]))
        copies.append(pltpu.make_async_copy(std.at[y], std_o.at[y], sem.at[1, y]))
    for copy in copies:
        copy.start()
    for copy in copies:
        copy.wait()


def body(tracer, mobility, source):
    sizes = tuple(lax.axis_size(a) for a in ("trial", "south", "east", "down"))
    Y, X, Z, L = tracer.shape
    downs, pairs = sizes[3], X // 2
    f32 = jnp.float32
    dma = pltpu.SemaphoreType.DMA
    result = pltpu.VMEM(tracer.shape, f32)
    anywhere = pl.BlockSpec(memory_space=pl.ANY)
    onchip = pl.BlockSpec(memory_space=pltpu.VMEM)
    standardized, final = pl.pallas_call(
        functools.partial(kernel, sizes),
        out_shape=(result, result),
        in_specs=[anywhere] * 3,
        out_specs=(onchip, onchip),
        scratch_shapes=[
            pltpu.VMEM((STEPS, Y + 2, X + 2, Z, L), f32),
            pltpu.VMEM((Y, X, Z, L), f32),
            pltpu.VMEM((Y, X, Z, L), f32),
            pltpu.VMEM((STEPS, 2, pairs, 2 * Y, L), f32),
            pltpu.VMEM((STEPS, 2, pairs, 2 * Y, L), f32),
            pltpu.VMEM((STEPS - 1, pairs, 2 * Y, L), f32),
            pltpu.VMEM((pairs, 2, 2 * Y, L), f32),
            pltpu.VMEM((pairs - DIRECT, 2, 2 * Y, L), f32),
            pltpu.VMEM((pairs - DIRECT, 2, 2 * Y, L), f32),
            pltpu.VMEM((pairs - DIRECT, 2, 2 * Y, L), f32),
            pltpu.VMEM((DIRECT, downs - 1, 2, 2 * Y, L), f32),
            pltpu.SemaphoreType.REGULAR((4,)),
            dma((Y + 2,)),
            dma,
            dma((STEPS, pairs)),
            dma,
            dma((STEPS,)),
            dma,
            dma((STEPS, pairs)),
            dma,
            dma((STEPS - 1, pairs)),
            dma((2 + DIRECT,)),
            dma((2 + DIRECT,)),
        ],
        compiler_params=pltpu.CompilerParams(
            collective_id=0, has_side_effects=True, vmem_limit_bytes=53 * 1024 * 1024
        ),
    )(tracer, mobility, source)
    shape = jax.ShapeDtypeStruct(tracer.shape, f32)
    return pl.pallas_call(
        put_out,
        out_shape=(shape, shape),
        in_specs=[onchip] * 2,
        out_specs=(anywhere, anywhere),
        scratch_shapes=[dma((2, Y))],
        compiler_params=pltpu.CompilerParams(vmem_limit_bytes=1024 * 1024),
    )(standardized, final)


def solution(mesh):
    spec = P(("trial", "south"), "east", "down", None)
    return jax.shard_map(
        body, mesh=mesh, in_specs=(spec,) * 3, out_specs=(spec,) * 2, check_vma=False
    )
```

```python
import functools

import jax
import jax.numpy as jnp
from jax import lax
from jax.experimental import pallas as pl
from jax.experimental.pallas import tpu as pltpu
from jax.sharding import PartitionSpec as P

STEPS = 3
FIRST = 4
AHEAD = 6
RELAY = 6
DIRECT = 2
MESH = pl.DeviceIdType.MESH


def kernel(
    sizes,
    tr, mo, so,
    st, end,
    u, m, s, zs, zr, rl, ms, mz, mc, my, mr,
    known, in_sem, s_send, s_recv, e_send, e_recv, z_send, z_recv, r_send, r_recv, m_send, m_recv,
):
    trials, souths, easts, downs = sizes
    Y, X, Z, L = tr.shape
    pairs = X // 2
    rows = 2 * Y
    at = {name: lax.axis_index(name) for name in ("trial", "south", "east", "down")}

    across = 2
    beside = 1 + at["down"] % 2 * 2

    def peer(name, count, shift):
        return {name: lax.rem(at[name] + shift + count, count)}

    def away(dy=0, dz=0):
        y = lax.rem(at["down"] % 2 * 2 + at["south"] // 2 + dy + 4, 4)
        z = lax.rem(at["down"] // 2 * trials + at["trial"] + dz + 2 * trials, 2 * trials)
        return {
            "trial": z % trials,
            "south": y % 2 * 2 + at["south"] % 2,
            "down": z // trials * 2 + y // 2,
        }

    def south(side, t, j, x):
        return pltpu.make_async_remote_copy(
            src_ref=u.at[t, Y if side else 1, x + 1],
            dst_ref=u.at[t, 0 if side else Y + 1, x + 1],
            send_sem=s_send,
            recv_sem=s_recv.at[t, j],
            device_id=peer("south", souths, 1 if side else -1),
            device_id_type=MESH,
        )

    def east(side, t):
        return pltpu.make_async_remote_copy(
            src_ref=u.at[t, pl.ds(1, Y), X if side else 1],
            dst_ref=u.at[t, pl.ds(1, Y), 0 if side else X + 1],
            send_sem=e_send,
            recv_sem=e_recv.at[t],
            device_id=peer("east", easts, 1 if side else -1),
            device_id_type=MESH,
        )

    def down(side, t, j):
        return pltpu.make_async_remote_copy(
            src_ref=zs.at[t, side, j],
            dst_ref=zr.at[t, side, j],
            send_sem=z_send,
            recv_sem=z_recv.at[t, j],
            device_id=peer("down", downs, 2 * side - 1),
            device_id_type=MESH,
        )

    early = at["down"] // 2 == 0
    inner = 1 - at["down"] % 2

    def hand(side, shift, t, j):
        return pltpu.make_async_remote_copy(
            src_ref=zs.at[t, side, j],
            dst_ref=rl.at[t - 1, side, j],
            send_sem=z_send,
            recv_sem=r_recv.at[t - 1, j],
            device_id=peer("down", downs, shift),
            device_id_type=MESH,
        )

    def forward(t, j):
        arrived(rl.at[t - 1, :, j], r_recv.at[t - 1, j])
        onward = pltpu.make_async_remote_copy(
            src_ref=rl.at[t - 1, :, j],
            dst_ref=zr.at[t, :, j],
            send_sem=r_send,
            recv_sem=z_recv.at[t, j],
            device_id=peer("down", downs, across),
            device_id_type=MESH,
        )
        onward.start()

    def faces(t, j):
        @pl.when(early)
        def _():
            down(inner, t, j).start()
            hand(1 - inner, beside, t, j).start()

        @pl.when(jnp.logical_not(early))
        def _():
            down(1 - inner, t, j).start()
            hand(inner, 1 - 2 * inner, t, j).start()

    merged = pairs - DIRECT

    def share(src, dst, d, i):
        return pltpu.make_async_remote_copy(
            src_ref=src,
            dst_ref=dst,
            send_sem=m_send.at[i],
            recv_sem=m_recv.at[i],
            device_id=peer("down", downs, d),
            device_id_type=MESH,
        )

    def south_pair(t, j):
        for side in (0, 1):
            for x in (j, X - 1 - j):
                south(side, t, j, x).start()

    def arrived(ref, sem):
        everything = pltpu.make_async_remote_copy(
            src_ref=ref, dst_ref=ref, send_sem=sem, recv_sem=sem,
            device_id=peer("south", souths, 1), device_id_type=MESH,
        )
        everything.wait_recv()

    loads = [
        pltpu.make_async_copy(tr.at[y], u.at[0, y + 1, pl.ds(1, X)], in_sem.at[y])
        for y in range(Y)
    ]
    for y in [0, Y - 1] + list(range(1, Y - 1)):
        loads[y].start()
    others = [
        pltpu.make_async_copy(mo, m, in_sem.at[Y]),
        pltpu.make_async_copy(so, s, in_sem.at[Y + 1]),
    ]
    for copy in others:
        copy.start()

    y_lo, y_hi = at["south"] // 2, at["down"] % 2
    z = at["down"] // 2 * trials + at["trial"]
    turn = 2 * trials - 2
    answers_below = jnp.logical_and(z >= 1, z <= turn)
    answers_above = z >= turn
    greeted = [
        (answers_below, away(dz=-1)),
        (answers_above, away(dz=1)),
        (y_hi == 1, away(dy=2 * y_lo - 1)),
    ]
    barrier = pltpu.get_barrier_semaphore()
    near = [peer("south", souths, d) for d in (-1, 1)]
    near += [peer("east", easts, d) for d in (-1, 1)]
    near += [away(dy=1 - 2 * y_lo)]
    for who in near:
        pl.semaphore_signal(barrier, inc=1, device_id=who, device_id_type=MESH)
    for answers, who in greeted:

        @pl.when(jnp.logical_not(answers))
        def _(who=who):
            pl.semaphore_signal(barrier, inc=1, device_id=who, device_id_type=MESH)

    below = (z + 2 * trials - 1) // (2 * trials) - z // (turn + 1)
    pl.semaphore_wait(barrier, len(near) + below + z // turn + y_hi)

    loads[0].wait()
    loads[Y - 1].wait()
    for j in range(FIRST):
        south_pair(0, j)
    for y in range(1, Y - 1):
        loads[y].wait()
    for side in (0, 1):
        east(side, 0).start()

    def first_faces(j, carry):
        for r, x in enumerate((j, X - 1 - j)):
            for y in range(Y):
                zs[0, 0, j, pl.ds(r * Y + y, 1), :] = u[0, y + 1, x + 1, pl.ds(0, 1), :]
                zs[0, 1, j, pl.ds(r * Y + y, 1), :] = u[0, y + 1, x + 1, pl.ds(Z - 1, 1), :]
        return carry

    lax.fori_loop(0, pairs, first_faces, 0)

    for answers, who in greeted:

        @pl.when(answers)
        def _(who=who):
            pl.semaphore_signal(known.at[4], inc=1, device_id=who, device_id_type=MESH)

    answers_due = 3 - below - z // turn - y_hi

    @pl.when(answers_due > 0)
    def _():
        pl.semaphore_wait(known.at[4], answers_due)

    rounds = ([away(dz=-1), away(dz=1)], [away(dz=-2)], [away(dy=-1)], [away(dy=-1)])
    for i, to in enumerate(rounds):
        for who in to:
            pl.semaphore_signal(known.at[i], inc=1, device_id=who, device_id_type=MESH)
        pl.semaphore_wait(known.at[i], len(to))

    def first_down(j, carry):
        for side in (0, 1):
            down(side, 0, j).start()
        return carry

    lax.fori_loop(0, pairs, first_down, 0)
    for j in range(FIRST, AHEAD):
        south_pair(0, j)
    for copy in others:
        copy.wait()

    level = lax.broadcasted_iota(jnp.int32, (Z, L), 0)
    top, bottom = level == 0, level == Z - 1

    def advance(t, j):
        arrived(zr.at[t, :, j], z_recv.at[t, j])
        arrived(u.at[t, 0, pl.ds(0, 4)], s_recv.at[t, j])

        @pl.when(j == 0)
        def _():
            arrived(u.at[t, pl.ds(1, Y), pl.ds(0, 2)], e_recv.at[t])

        for r, x in enumerate((j, X - 1 - j)):
            for y in range(Y):
                at_row = pl.ds(r * Y + y, 1)
                middle = u[t, y + 1, x + 1]
                before = jnp.where(top, zr[t, 1, j, at_row, :], pltpu.roll(middle, 1, 0))
                after = jnp.where(bottom, zr[t, 0, j, at_row, :], pltpu.roll(middle, Z - 1, 0))
                spread = u[t, y, x + 1] + u[t, y + 2, x + 1] + u[t, y + 1, x] + u[t, y + 1, x + 2]
                spread = spread + before + after - 6.0 * middle
                value = middle + m[y, x] * spread + s[y, x]
                if t + 1 < STEPS:
                    u[t + 1, y + 1, x + 1] = value
                    zs[t + 1, 0, j, at_row, :] = value[:1]
                    zs[t + 1, 1, j, at_row, :] = value[Z - 1 :]
                else:
                    end[y, x] = value
                    mean = jnp.sum(value, axis=0, keepdims=True) * (1.0 / Z)
                    off = value - mean
                    ms[j, 0, at_row, :] = mean
                    ms[j, 1, at_row, :] = jnp.sum(off * off, axis=0, keepdims=True)

    def finish(j, mean, spreads):
        scale = lax.rsqrt(spreads * (1.0 / (Z * downs)) + 0.0001)
        for r, x in enumerate((j, X - 1 - j)):
            for y in range(Y):
                k = r * Y + y
                st[y, x] = (end[y, x] - mean[k : k + 1]) * scale[k : k + 1]

    for t in range(STEPS):

        def step(j, carry, t=t):
            n = t * pairs + j - RELAY

            @pl.when(jnp.logical_and(early, jnp.logical_and(n >= 0, n < (STEPS - 1) * pairs)))
            def _():
                forward(n // pairs + 1, n % pairs)

            advance(t, j)
            if t + 1 < STEPS:
                faces(t + 1, j)

                @pl.when(j == 0)
                def _():
                    for side in (0, 1):
                        east(side, t + 1).start()

                n = t * pairs + j + AHEAD
                south_pair(n // pairs, n % pairs)
            else:

                @pl.when(j < merged)
                def _():
                    share(ms.at[j], mz.at[j], across, 0).start()

                @pl.when(j >= merged)
                def _():
                    k = j - merged
                    for d in range(1, downs):
                        share(ms.at[j], mr.at[k, d - 1], d, 2 + k).start()

                @pl.when(j + AHEAD < pairs)
                def _():
                    south_pair(t, j + AHEAD)

            return carry

        lax.fori_loop(0, pairs, step, 0)

    arrived(mz, m_recv.at[0])

    def merge(j, carry):
        gap = ms[j, 0] - mz[j, 0]
        mc[j, 0] = (ms[j, 0] + mz[j, 0]) * 0.5
        mc[j, 1] = ms[j, 1] + mz[j, 1] + gap * gap * (0.5 * Z)
        return carry

    lax.fori_loop(0, merged, merge, 0)
    share(mc, my, beside, 1).start()
    arrived(my, m_recv.at[1])

    def finish_merged(j, carry):
        gap = mc[j, 0] - my[j, 0]
        finish(j, (mc[j, 0] + my[j, 0]) * 0.5, mc[j, 1] + my[j, 1] + gap * gap * (1.0 * Z))
        return carry

    lax.fori_loop(0, merged, finish_merged, 0)

    def finish_direct(k, carry):
        j = merged + k
        arrived(mr.at[k], m_recv.at[2 + k])
        means = [ms[j, 0]] + [mr[k, d, 0] for d in range(downs - 1)]
        mean = functools.reduce(jnp.add, means) * (1.0 / downs)
        spreads = functools.reduce(jnp.add, [ms[j, 1]] + [mr[k, d, 1] for d in range(downs - 1)])
        between = functools.reduce(jnp.add, [(a - mean) * (a - mean) for a in means])
        finish(j, mean, spreads + between * Z)
        return carry

    lax.fori_loop(0, DIRECT, finish_direct, 0)

    arrived(u.at[:, pl.ds(0, 2), pl.ds(1, X)], s_send)
    arrived(u.at[:, pl.ds(0, 2), pl.ds(0, Y)], e_send)
    arrived(zs, z_send)

    @pl.when(early)
    def _():
        arrived(rl, r_send)

    for i, ref in enumerate([mz, my] + [mr.at[k] for k in range(DIRECT)]):
        arrived(ref, m_send.at[i])


def put_out(std, end, std_o, end_o, sem):
    copies = []
    for y in range(std.shape[0]):
        copies.append(pltpu.make_async_copy(end.at[y], end_o.at[y], sem.at[0, y]))
        copies.append(pltpu.make_async_copy(std.at[y], std_o.at[y], sem.at[1, y]))
    for copy in copies:
        copy.start()
    for copy in copies:
        copy.wait()


def body(tracer, mobility, source):
    sizes = tuple(lax.axis_size(a) for a in ("trial", "south", "east", "down"))
    Y, X, Z, L = tracer.shape
    downs, pairs = sizes[3], X // 2
    f32 = jnp.float32
    dma = pltpu.SemaphoreType.DMA
    result = pltpu.VMEM(tracer.shape, f32)
    anywhere = pl.BlockSpec(memory_space=pl.ANY)
    onchip = pl.BlockSpec(memory_space=pltpu.VMEM)
    standardized, final = pl.pallas_call(
        functools.partial(kernel, sizes),
        out_shape=(result, result),
        in_specs=[anywhere] * 3,
        out_specs=(onchip, onchip),
        scratch_shapes=[
            pltpu.VMEM((STEPS, Y + 2, X + 2, Z, L), f32),
            pltpu.VMEM((Y, X, Z, L), f32),
            pltpu.VMEM((Y, X, Z, L), f32),
            pltpu.VMEM((STEPS, 2, pairs, 2 * Y, L), f32),
            pltpu.VMEM((STEPS, 2, pairs, 2 * Y, L), f32),
            pltpu.VMEM((STEPS - 1, 2, pairs, 2 * Y, L), f32),
            pltpu.VMEM((pairs, 2, 2 * Y, L), f32),
            pltpu.VMEM((pairs - DIRECT, 2, 2 * Y, L), f32),
            pltpu.VMEM((pairs - DIRECT, 2, 2 * Y, L), f32),
            pltpu.VMEM((pairs - DIRECT, 2, 2 * Y, L), f32),
            pltpu.VMEM((DIRECT, downs - 1, 2, 2 * Y, L), f32),
            pltpu.SemaphoreType.REGULAR((5,)),
            dma((Y + 2,)),
            dma,
            dma((STEPS, pairs)),
            dma,
            dma((STEPS,)),
            dma,
            dma((STEPS, pairs)),
            dma,
            dma((STEPS - 1, pairs)),
            dma((2 + DIRECT,)),
            dma((2 + DIRECT,)),
        ],
        compiler_params=pltpu.CompilerParams(
            collective_id=0, has_side_effects=True, vmem_limit_bytes=53 * 1024 * 1024
        ),
    )(tracer, mobility, source)
    shape = jax.ShapeDtypeStruct(tracer.shape, f32)
    return pl.pallas_call(
        put_out,
        out_shape=(shape, shape),
        in_specs=[onchip] * 2,
        out_specs=(anywhere, anywhere),
        scratch_shapes=[dma((2, Y))],
        compiler_params=pltpu.CompilerParams(vmem_limit_bytes=1024 * 1024),
    )(standardized, final)


def solution(mesh):
    spec = P(("trial", "south"), "east", "down", None)
    return jax.shard_map(
        body, mesh=mesh, in_specs=(spec,) * 3, out_specs=(spec,) * 2, check_vma=False
    )
```

```python
import functools

import jax
import jax.numpy as jnp
from jax import lax
from jax.experimental import pallas as pl
from jax.experimental.pallas import tpu as pltpu
from jax.sharding import PartitionSpec as P

STEPS = 3
FIRST = 4
AHEAD = 6
RELAY = 6
DIRECT = 2
MESH = pl.DeviceIdType.MESH


def kernel(
    sizes,
    tr, mo, so,
    st, end,
    u, m, s, zs, zr, rl, ms, mz, mc, my, mr,
    known, in_sem, s_send, s_recv, e_send, e_recv, z_send, z_recv, r_send, r_recv, m_send, m_recv,
):
    trials, souths, easts, downs = sizes
    Y, X, Z, L = tr.shape
    pairs = X // 2
    rows = 2 * Y
    at = {name: lax.axis_index(name) for name in ("trial", "south", "east", "down")}

    across = 2
    beside = 1 + at["down"] % 2 * 2

    def peer(name, count, shift):
        return {name: lax.rem(at[name] + shift + count, count)}

    def away(dy=0, dz=0):
        y = lax.rem(at["down"] % 2 * 2 + at["south"] // 2 + dy + 4, 4)
        z = lax.rem(at["down"] // 2 * trials + at["trial"] + dz + 2 * trials, 2 * trials)
        return {
            "trial": z % trials,
            "south": y % 2 * 2 + at["south"] % 2,
            "down": z // trials * 2 + y // 2,
        }

    def south(side, t, j, x):
        return pltpu.make_async_remote_copy(
            src_ref=u.at[t, Y if side else 1, x + 1],
            dst_ref=u.at[t, 0 if side else Y + 1, x + 1],
            send_sem=s_send,
            recv_sem=s_recv.at[t, j],
            device_id=peer("south", souths, 1 if side else -1),
            device_id_type=MESH,
        )

    def east(side, t):
        return pltpu.make_async_remote_copy(
            src_ref=u.at[t, pl.ds(1, Y), X if side else 1],
            dst_ref=u.at[t, pl.ds(1, Y), 0 if side else X + 1],
            send_sem=e_send,
            recv_sem=e_recv.at[t],
            device_id=peer("east", easts, 1 if side else -1),
            device_id_type=MESH,
        )

    def down(side, t, j):
        return pltpu.make_async_remote_copy(
            src_ref=zs.at[t, side, j],
            dst_ref=zr.at[t, side, j],
            send_sem=z_send,
            recv_sem=z_recv.at[t, j],
            device_id=peer("down", downs, 2 * side - 1),
            device_id_type=MESH,
        )

    early = at["down"] // 2 == 0
    inner = 1 - at["down"] % 2

    def hand(side, shift, t, j):
        return pltpu.make_async_remote_copy(
            src_ref=zs.at[t, side, j],
            dst_ref=rl.at[t - 1, side, j],
            send_sem=z_send,
            recv_sem=r_recv.at[t - 1, j],
            device_id=peer("down", downs, shift),
            device_id_type=MESH,
        )

    def forward(t, j):
        arrived(rl.at[t - 1, :, j], r_recv.at[t - 1, j])
        onward = pltpu.make_async_remote_copy(
            src_ref=rl.at[t - 1, :, j],
            dst_ref=zr.at[t, :, j],
            send_sem=r_send,
            recv_sem=z_recv.at[t, j],
            device_id=peer("down", downs, across),
            device_id_type=MESH,
        )
        onward.start()

    def faces(t, j):
        @pl.when(early)
        def _():
            down(inner, t, j).start()
            hand(1 - inner, beside, t, j).start()

        @pl.when(jnp.logical_not(early))
        def _():
            down(1 - inner, t, j).start()
            hand(inner, 1 - 2 * inner, t, j).start()

    merged = pairs - DIRECT

    def share(src, dst, d, i):
        return pltpu.make_async_remote_copy(
            src_ref=src,
            dst_ref=dst,
            send_sem=m_send.at[i],
            recv_sem=m_recv.at[i],
            device_id=peer("down", downs, d),
            device_id_type=MESH,
        )

    def south_pair(t, j):
        for side in (0, 1):
            for x in (j, X - 1 - j):
                south(side, t, j, x).start()

    def arrived(ref, sem):
        everything = pltpu.make_async_remote_copy(
            src_ref=ref, dst_ref=ref, send_sem=sem, recv_sem=sem,
            device_id=peer("south", souths, 1), device_id_type=MESH,
        )
        everything.wait_recv()

    def load(y, x, count, i):
        return pltpu.make_async_copy(
            tr.at[y, pl.ds(x, count)], u.at[0, y + 1, pl.ds(x + 1, count)], in_sem.at[i]
        )

    sent = (0, Y - 1)
    first = [load(y, x, 1, Y + 2 + 2 * a + b) for a, y in enumerate(sent) for b, x in enumerate((0, X - 1))]
    for copy in first:
        copy.start()
    loads = [load(y, 1, X - 2, y) if y in sent else load(y, 0, X, y) for y in range(Y)]
    for y in [0, Y - 1] + list(range(1, Y - 1)):
        loads[y].start()
    others = [
        pltpu.make_async_copy(mo, m, in_sem.at[Y]),
        pltpu.make_async_copy(so, s, in_sem.at[Y + 1]),
    ]
    for copy in others:
        copy.start()

    y_lo, y_hi = at["south"] // 2, at["down"] % 2
    z = at["down"] // 2 * trials + at["trial"]
    turn = 2 * trials - 2
    answers_below = jnp.logical_and(z >= 1, z <= turn)
    answers_above = z >= turn
    greeted = [
        (answers_below, away(dz=-1)),
        (answers_above, away(dz=1)),
        (y_hi == 1, away(dy=2 * y_lo - 1)),
    ]
    barrier = pltpu.get_barrier_semaphore()
    near = [peer("south", souths, d) for d in (-1, 1)]
    near += [peer("east", easts, d) for d in (-1, 1)]
    near += [away(dy=1 - 2 * y_lo)]
    for who in near:
        pl.semaphore_signal(barrier, inc=1, device_id=who, device_id_type=MESH)
    for answers, who in greeted:

        @pl.when(jnp.logical_not(answers))
        def _(who=who):
            pl.semaphore_signal(barrier, inc=1, device_id=who, device_id_type=MESH)

    below = (z + 2 * trials - 1) // (2 * trials) - z // (turn + 1)
    pl.semaphore_wait(barrier, len(near) + below + z // turn + y_hi)

    for copy in first:
        copy.wait()
    south_pair(0, 0)
    loads[0].wait()
    loads[Y - 1].wait()
    for j in range(1, FIRST):
        south_pair(0, j)
    for y in range(1, Y - 1):
        loads[y].wait()
    for side in (0, 1):
        east(side, 0).start()

    def first_faces(j, carry):
        for r, x in enumerate((j, X - 1 - j)):
            for y in range(Y):
                zs[0, 0, j, pl.ds(r * Y + y, 1), :] = u[0, y + 1, x + 1, pl.ds(0, 1), :]
                zs[0, 1, j, pl.ds(r * Y + y, 1), :] = u[0, y + 1, x + 1, pl.ds(Z - 1, 1), :]
        return carry

    lax.fori_loop(0, pairs, first_faces, 0)

    for answers, who in greeted:

        @pl.when(answers)
        def _(who=who):
            pl.semaphore_signal(known.at[4], inc=1, device_id=who, device_id_type=MESH)

    answers_due = 3 - below - z // turn - y_hi

    @pl.when(answers_due > 0)
    def _():
        pl.semaphore_wait(known.at[4], answers_due)

    rounds = ([away(dz=-1), away(dz=1)], [away(dz=-2)], [away(dy=-1)], [away(dy=-1)])
    for i, to in enumerate(rounds):
        for who in to:
            pl.semaphore_signal(known.at[i], inc=1, device_id=who, device_id_type=MESH)
        pl.semaphore_wait(known.at[i], len(to))

    def first_down(j, carry):
        for side in (0, 1):
            down(side, 0, j).start()
        return carry

    lax.fori_loop(0, pairs, first_down, 0)
    for j in range(FIRST, AHEAD):
        south_pair(0, j)
    for copy in others:
        copy.wait()

    level = lax.broadcasted_iota(jnp.int32, (Z, L), 0)
    top, bottom = level == 0, level == Z - 1

    def advance(t, j):
        arrived(zr.at[t, :, j], z_recv.at[t, j])
        arrived(u.at[t, 0, pl.ds(0, 4)], s_recv.at[t, j])

        @pl.when(j == 0)
        def _():
            arrived(u.at[t, pl.ds(1, Y), pl.ds(0, 2)], e_recv.at[t])

        for r, x in enumerate((j, X - 1 - j)):
            for y in range(Y):
                at_row = pl.ds(r * Y + y, 1)
                middle = u[t, y + 1, x + 1]
                before = jnp.where(top, zr[t, 1, j, at_row, :], pltpu.roll(middle, 1, 0))
                after = jnp.where(bottom, zr[t, 0, j, at_row, :], pltpu.roll(middle, Z - 1, 0))
                spread = u[t, y, x + 1] + u[t, y + 2, x + 1] + u[t, y + 1, x] + u[t, y + 1, x + 2]
                spread = spread + before + after - 6.0 * middle
                value = middle + m[y, x] * spread + s[y, x]
                if t + 1 < STEPS:
                    u[t + 1, y + 1, x + 1] = value
                    zs[t + 1, 0, j, at_row, :] = value[:1]
                    zs[t + 1, 1, j, at_row, :] = value[Z - 1 :]
                else:
                    end[y, x] = value
                    mean = jnp.sum(value, axis=0, keepdims=True) * (1.0 / Z)
                    off = value - mean
                    ms[j, 0, at_row, :] = mean
                    ms[j, 1, at_row, :] = jnp.sum(off * off, axis=0, keepdims=True)

    def finish(j, mean, spreads):
        scale = lax.rsqrt(spreads * (1.0 / (Z * downs)) + 0.0001)
        for r, x in enumerate((j, X - 1 - j)):
            for y in range(Y):
                k = r * Y + y
                st[y, x] = (end[y, x] - mean[k : k + 1]) * scale[k : k + 1]

    for t in range(STEPS):

        def step(j, carry, t=t):
            n = t * pairs + j - RELAY

            @pl.when(jnp.logical_and(early, jnp.logical_and(n >= 0, n < (STEPS - 1) * pairs)))
            def _():
                forward(n // pairs + 1, n % pairs)

            advance(t, j)
            if t + 1 < STEPS:
                faces(t + 1, j)

                @pl.when(j == 0)
                def _():
                    for side in (0, 1):
                        east(side, t + 1).start()

                n = t * pairs + j + AHEAD
                south_pair(n // pairs, n % pairs)
            else:

                @pl.when(j < merged)
                def _():
                    share(ms.at[j], mz.at[j], across, 0).start()

                @pl.when(j >= merged)
                def _():
                    k = j - merged
                    for d in range(1, downs):
                        share(ms.at[j], mr.at[k, d - 1], d, 2 + k).start()

                @pl.when(j + AHEAD < pairs)
                def _():
                    south_pair(t, j + AHEAD)

            return carry

        lax.fori_loop(0, pairs, step, 0)

    arrived(mz, m_recv.at[0])

    def merge(j, carry):
        gap = ms[j, 0] - mz[j, 0]
        mc[j, 0] = (ms[j, 0] + mz[j, 0]) * 0.5
        mc[j, 1] = ms[j, 1] + mz[j, 1] + gap * gap * (0.5 * Z)
        return carry

    lax.fori_loop(0, merged, merge, 0)
    share(mc, my, beside, 1).start()
    arrived(my, m_recv.at[1])

    def finish_merged(j, carry):
        gap = mc[j, 0] - my[j, 0]
        finish(j, (mc[j, 0] + my[j, 0]) * 0.5, mc[j, 1] + my[j, 1] + gap * gap * (1.0 * Z))
        return carry

    lax.fori_loop(0, merged, finish_merged, 0)

    def finish_direct(k, carry):
        j = merged + k
        arrived(mr.at[k], m_recv.at[2 + k])
        means = [ms[j, 0]] + [mr[k, d, 0] for d in range(downs - 1)]
        mean = functools.reduce(jnp.add, means) * (1.0 / downs)
        spreads = functools.reduce(jnp.add, [ms[j, 1]] + [mr[k, d, 1] for d in range(downs - 1)])
        between = functools.reduce(jnp.add, [(a - mean) * (a - mean) for a in means])
        finish(j, mean, spreads + between * Z)
        return carry

    lax.fori_loop(0, DIRECT, finish_direct, 0)

    arrived(u.at[:, pl.ds(0, 2), pl.ds(1, X)], s_send)
    arrived(u.at[:, pl.ds(0, 2), pl.ds(0, Y)], e_send)
    arrived(zs, z_send)

    @pl.when(early)
    def _():
        arrived(rl, r_send)

    for i, ref in enumerate([mz, my] + [mr.at[k] for k in range(DIRECT)]):
        arrived(ref, m_send.at[i])


def put_out(std, end, std_o, end_o, sem):
    copies = []
    for y in range(std.shape[0]):
        copies.append(pltpu.make_async_copy(end.at[y], end_o.at[y], sem.at[0, y]))
        copies.append(pltpu.make_async_copy(std.at[y], std_o.at[y], sem.at[1, y]))
    for copy in copies:
        copy.start()
    for copy in copies:
        copy.wait()


def body(tracer, mobility, source):
    sizes = tuple(lax.axis_size(a) for a in ("trial", "south", "east", "down"))
    Y, X, Z, L = tracer.shape
    downs, pairs = sizes[3], X // 2
    f32 = jnp.float32
    dma = pltpu.SemaphoreType.DMA
    result = pltpu.VMEM(tracer.shape, f32)
    anywhere = pl.BlockSpec(memory_space=pl.ANY)
    onchip = pl.BlockSpec(memory_space=pltpu.VMEM)
    standardized, final = pl.pallas_call(
        functools.partial(kernel, sizes),
        out_shape=(result, result),
        in_specs=[anywhere] * 3,
        out_specs=(onchip, onchip),
        scratch_shapes=[
            pltpu.VMEM((STEPS, Y + 2, X + 2, Z, L), f32),
            pltpu.VMEM((Y, X, Z, L), f32),
            pltpu.VMEM((Y, X, Z, L), f32),
            pltpu.VMEM((STEPS, 2, pairs, 2 * Y, L), f32),
            pltpu.VMEM((STEPS, 2, pairs, 2 * Y, L), f32),
            pltpu.VMEM((STEPS - 1, 2, pairs, 2 * Y, L), f32),
            pltpu.VMEM((pairs, 2, 2 * Y, L), f32),
            pltpu.VMEM((pairs - DIRECT, 2, 2 * Y, L), f32),
            pltpu.VMEM((pairs - DIRECT, 2, 2 * Y, L), f32),
            pltpu.VMEM((pairs - DIRECT, 2, 2 * Y, L), f32),
            pltpu.VMEM((DIRECT, downs - 1, 2, 2 * Y, L), f32),
            pltpu.SemaphoreType.REGULAR((5,)),
            dma((Y + 6,)),
            dma,
            dma((STEPS, pairs)),
            dma,
            dma((STEPS,)),
            dma,
            dma((STEPS, pairs)),
            dma,
            dma((STEPS - 1, pairs)),
            dma((2 + DIRECT,)),
            dma((2 + DIRECT,)),
        ],
        compiler_params=pltpu.CompilerParams(
            collective_id=0, has_side_effects=True, vmem_limit_bytes=53 * 1024 * 1024
        ),
    )(tracer, mobility, source)
    shape = jax.ShapeDtypeStruct(tracer.shape, f32)
    return pl.pallas_call(
        put_out,
        out_shape=(shape, shape),
        in_specs=[onchip] * 2,
        out_specs=(anywhere, anywhere),
        scratch_shapes=[dma((2, Y))],
        compiler_params=pltpu.CompilerParams(vmem_limit_bytes=1024 * 1024),
    )(standardized, final)


def solution(mesh):
    spec = P(("trial", "south"), "east", "down", None)
    return jax.shard_map(
        body, mesh=mesh, in_specs=(spec,) * 3, out_specs=(spec,) * 2, check_vma=False
    )
```
